32 devices in a mesh: fsdp: 8 (over z, x), rep: 4 (over y, core).
Axes of the slice: x: 2, y: 2, z: 4, core: 2. Of those that a mesh axis runs over, the one named last changes fastest.
Arguments:
- cross_base: bfloat16 [4096, 4096], P(('fsdp', 'rep')), may hold values from -6 to 6
- layer_in: bfloat16 [4096, 4096], P(('fsdp', 'rep')), may hold values from -6 to 6
- grad_out: bfloat16 [4096, 4096], P(('fsdp', 'rep')), may hold values from -6 to 6
- reduce_a: bfloat16 [4096, 256], P('fsdp'), may hold values from -0.09375 to 0.09375
- expand_a: bfloat16 [4096, 256], P('fsdp'), may hold values from -0.375 to 0.375
- reduce_b: bfloat16 [4096, 256], P('fsdp'), may hold values from -0.09375 to 0.09375
- expand_b: bfloat16 [4096, 256], P('fsdp'), may hold values from -0.375 to 0.375
Outputs:
- grad_layer_in: bfloat16 [4096, 4096], P(('fsdp', 'rep'))
- grad_base: bfloat16 [4096, 4096], P(('fsdp', 'rep'))
- grad_reduce_a: float32 [4096, 256], P('fsdp')
- grad_expand_a: float32 [4096, 256], P('fsdp')
- grad_reduce_b: float32 [4096, 256], P('fsdp')
- grad_expand_b: float32 [4096, 256], P('fsdp')
The draws below stay inside these ranges and needn't reach their ends.
All inputs are finite; a program needn't handle non-finite values.
Results may differ from the reference program's by a relative error of at most 0.015.
Values may be sent and summed in bfloat16 or wider, within the bound.
No kernel may reach another device: no remote copies, remote signals or barrier semaphores. Data moves between devices by JAX's collectives and lax.ppermute only.
A program may use at most 128 MiB of HBM per device.

```python
import math
import jax
import jax.numpy as jnp
from jax import lax

D = 4096
RANK = 256
TOKENS = 4096


def with_spikes(array, own_key, source, target, parts, factor):
    owner, partner = [(jnp.arange(array.shape[position]) // (array.shape[position] // parts)).reshape([-1 if axis == position else 1 for axis in range(array.ndim)]) for position in (source, target)]
    chosen = jax.random.permutation(own_key, parts)[partner]
    strong = (owner == chosen) | (owner == (partner + parts // 2) % parts)
    return jnp.where(strong, factor * array, array)


def block_scale(key, extent, split, smallest, largest):
    factor_of, own = 1.0, jax.random.fold_in(key, 6)
    for dim, parts in split:
        heights = jnp.exp(jax.random.uniform(jax.random.fold_in(own, dim), (parts,), jnp.float32, smallest / len(split), largest / len(split)))
        factor_of = factor_of * jnp.repeat(heights, extent[dim] // parts).reshape([-1 if axis == dim else 1 for axis in range(len(extent))])
    return factor_of


def gaussian(stream_key, dims, scale, most, pieces=(), kind=jnp.bfloat16):
    level = block_scale(stream_key, dims, pieces, -0.22, 0.18) if pieces else 1.0
    drawn = jax.random.normal(stream_key, dims, jnp.float32) * scale * level
    return jnp.minimum(jnp.maximum(drawn, -most), most).astype(kind)


def gaussian_with(own_key, shape, width, reach, pieces, heavy, held_as=jnp.bfloat16):
    result = width * jax.random.normal(own_key, shape, jnp.float32)
    if pieces:
        result = result * block_scale(own_key, shape, pieces, -0.22, 0.18)
    return jnp.clip(with_spikes(result, jax.random.fold_in(own_key, 3), *heavy), -reach, reach).astype(held_as)


def setup_inputs(seed: int = 0) -> dict:
    splits = jax.random.split(jax.random.key(seed), 8)
    return {
        "cross_base": gaussian(splits[0], (TOKENS, D), 1.0, 6.0, ((0, 32),)),
        "layer_in": gaussian(splits[1], (TOKENS, D), 1.0, 6.0, ((0, 32),)),
        "grad_out": gaussian_with(splits[2], (TOKENS, D), 1.0, 6.0, ((0, 32),), (0, 1, 32, 2.75)),
        "reduce_a": gaussian(splits[3], (D, RANK), D ** -0.5, 0.09375, ((0, 8),)),
        "expand_a": gaussian(splits[4], (D, RANK), RANK ** -0.5, 0.375, ((0, 8),)),
        "reduce_b": gaussian(splits[5], (D, RANK), D ** -0.5, 0.09375, ((0, 8),)),
        "expand_b": gaussian(splits[6], (D, RANK), RANK ** -0.5, 0.375, ((0, 8),)),
    }


def contract_rows(left, right):
    return lax.dot_general(left, right, (((0,), (0,)), ((), ())), preferred_element_type=jnp.float32)

def contract_cols(left, right):
    return lax.dot_general(left, right, (((1,), (1,)), ((), ())), preferred_element_type=jnp.float32)

def project(inputs, reduce_full, expand_full):
    narrow = jnp.dot(inputs, reduce_full, preferred_element_type=jnp.float32).astype(jnp.bfloat16)
    return (narrow, contract_cols(narrow, expand_full))

def local_backward(grad_in, cross_base, reduce_full, expand_full):
    grad_wide = grad_in.astype(jnp.float32)
    masked = (grad_wide * cross_base.astype(jnp.float32)).astype(jnp.bfloat16)
    narrow_grad = jnp.dot(masked, expand_full, preferred_element_type=jnp.float32).astype(jnp.bfloat16)
    passed = grad_wide + contract_cols(narrow_grad, reduce_full)
    return (masked, narrow_grad, passed)

def reference(cross_base, layer_in, grad_out, reduce_a, expand_a, reduce_b, expand_b):
    factor = 1.0 / math.sqrt(TOKENS)
    base_wide = cross_base.astype(jnp.float32)
    narrow_a, cross_a = project(layer_in, reduce_a, expand_a)
    middle = (layer_in.astype(jnp.float32) + base_wide * cross_a).astype(jnp.bfloat16)
    narrow_b, cross_b = project(middle, reduce_b, expand_b)
    masked_b, narrow_grad_b, passed_b = local_backward(grad_out, cross_base, reduce_b, expand_b)
    grad_expand_b = contract_rows(masked_b, narrow_b) * factor
    grad_reduce_b = contract_rows(middle, narrow_grad_b) * factor
    grad_middle = passed_b.astype(jnp.bfloat16)
    masked_a, narrow_grad_a, passed_a = local_backward(grad_middle, cross_base, reduce_a, expand_a)
    grad_expand_a = contract_rows(masked_a, narrow_a) * factor
    grad_reduce_a = contract_rows(layer_in, narrow_grad_a) * factor
    grad_layer_in = passed_a.astype(jnp.bfloat16)
    grad_base = (grad_out.astype(jnp.float32) * cross_b + grad_middle.astype(jnp.float32) * cross_a).astype(jnp.bfloat16)
    return (grad_layer_in, grad_base, grad_reduce_a, grad_expand_a, grad_reduce_b, grad_expand_b)
```

```python
import math

import jax
import jax.numpy as jnp
from jax import lax
from jax.sharding import PartitionSpec as P


BF16 = jnp.bfloat16
F32 = jnp.float32


def contract_rows(left, right):
    return lax.dot_general(
        left, right, (((0,), (0,)), ((), ())), preferred_element_type=F32
    )


def contract_cols(left, right):
    return lax.dot_general(
        left, right, (((1,), (1,)), ((), ())), preferred_element_type=F32
    )


def matmul(left, right):
    return jnp.dot(left, right, preferred_element_type=F32)


def swap(value, axis, mask):
    size = lax.axis_size(axis)
    return lax.ppermute(value, axis, [(i, i ^ mask) for i in range(size)])


class Grid:
    def __init__(self):
        fsdp, rep = lax.axis_index("fsdp"), lax.axis_index("rep")
        self.steps = {"x": ("fsdp", 1, 2), "y": ("rep", 2, 2), "c": ("rep", 1, 2)}
        self.index = {"x": fsdp % 2, "y": rep // 2, "c": rep % 2}
        self.z = []
        scale, left = 2, lax.axis_size("fsdp") // 2
        while left > 1:
            count = 4 if left % 4 == 0 else 2
            name = f"z{len(self.z)}"
            self.steps[name] = ("fsdp", scale, count)
            self.index[name] = (fsdp // scale) % count
            self.z.append(name)
            scale, left = scale * count, left // count
        dims = self.z[::-1] + ["x", "y"]
        self.dim = {name: place for place, name in enumerate(dims)}
        self.shape = tuple(self.steps[name][2] for name in dims)

    def order(self, letters):
        return [name for letter in letters for name in (self.z if letter == "z" else [letter])]

    def exchange(self, value, direction, mask):
        axis, scale, _ = self.steps[direction]
        return swap(value, axis, mask * scale)


def in_order(pieces, index):
    bit = 1
    while bit < len(pieces):
        odd = (index & bit) != 0
        pieces = [
            jnp.where(odd, pieces[k ^ bit], pieces[k]) for k in range(len(pieces))
        ]
        bit *= 2
    return pieces


def gather(grid, piece, order):
    block = piece.reshape((1,) * len(grid.shape) + piece.shape)
    for direction in grid.order(order):
        count = grid.steps[direction][2]
        pieces = [block] + [grid.exchange(block, direction, k) for k in range(1, count)]
        block = jnp.concatenate(in_order(pieces, grid.index[direction]), axis=grid.dim[direction])
    return block


def scatter(grid, partial, order):
    block = partial
    for direction in grid.order(order):
        count, dim = grid.steps[direction][2], grid.dim[direction]
        parts = [lax.slice_in_dim(block, k, k + 1, axis=dim) for k in range(count)]
        parts = in_order(parts, grid.index[direction])
        total = parts[0].astype(F32)
        for k in range(1, count):
            total = total + grid.exchange(parts[k].astype(BF16), direction, k).astype(F32)
        block = total
    return block.reshape(block.shape[-2:])


def halves(value, chunks):
    width = value.shape[1] // (2 * chunks)
    cut = [value[:, k * width : (k + 1) * width] for k in range(2 * chunks)]
    return jnp.concatenate(cut[0::2], axis=1), jnp.concatenate(cut[1::2], axis=1)


def on_device(cross_base, layer_in, grad_out, reduce_a, expand_a, reduce_b, expand_b):
    grid = Grid()
    fsdp = lax.axis_size("fsdp")
    rows = cross_base.shape[0]
    shard, rank = reduce_a.shape
    factor = 1.0 / math.sqrt(rows * fsdp * lax.axis_size("rep"))
    core, y = grid.index["c"], grid.index["y"]
    first = core == 0

    def quarter(weight):
        return lax.dynamic_slice_in_dim(weight, (core * 2 + y) * (shard // 4), shard // 4, 0)

    def gathered(weight, order):
        full = gather(grid, quarter(weight), order)
        return full.reshape(-1, rank)

    def spread_in(value):
        low, high = halves(value, fsdp)
        mine, other = jnp.where(first, low, high), jnp.where(first, high, low)
        return jnp.concatenate([mine, grid.exchange(other, "c", 1)], axis=0)

    def spread_out(value):
        mine, other = value[:rows], grid.exchange(value[rows:], "c", 1)
        low, high = jnp.where(first, mine, other), jnp.where(first, other, mine)
        width = low.shape[1] // fsdp
        cut = [
            part[:, k * width : (k + 1) * width] for k in range(fsdp) for part in (low, high)
        ]
        return jnp.concatenate(cut, axis=1)

    def over_cores(partial):
        other = grid.exchange(partial, "c", 1)
        return (partial + jnp.concatenate([other[rows:], other[:rows]], axis=0)).astype(BF16)

    def reduced(masked_like, narrow_like, order):
        partial = contract_rows(masked_like, narrow_like)
        partial = partial.reshape(*grid.shape, shard // 4, rank)
        part = (scatter(grid, partial, order)).astype(BF16)
        pair = in_order([part, grid.exchange(part, "y", 1)], y)
        both = jnp.concatenate(pair, axis=0)
        quad = in_order([both, grid.exchange(both, "c", 1)], core)
        return jnp.concatenate(quad, axis=0).astype(F32) * factor

    layer = spread_in(layer_in)
    base = spread_in(cross_base)
    grad = spread_in(grad_out)
    w_ra = gathered(reduce_a, "zxy")
    w_ea = gathered(expand_a, "zyx")
    w_rb = gathered(reduce_b, "xzy")
    w_eb = gathered(expand_b, "yzx")

    base_wide, grad_wide = base.astype(F32), grad.astype(F32)
    narrow_a = over_cores(matmul(layer, w_ra))
    cross_a = contract_cols(narrow_a, w_ea)
    middle = (layer.astype(F32) + base_wide * cross_a).astype(BF16)
    narrow_b = over_cores(matmul(middle, w_rb))
    masked_b = (grad_wide * base_wide).astype(BF16)
    grad_eb = reduced(masked_b, narrow_b, "yxz")
    narrow_grad_b = over_cores(matmul(masked_b, w_eb))
    grad_rb = reduced(middle, narrow_grad_b, "xyz")
    grad_middle = (grad_wide + contract_cols(narrow_grad_b, w_rb)).astype(BF16)
    middle_wide = grad_middle.astype(F32)
    masked_a = (middle_wide * base_wide).astype(BF16)
    grad_ea = reduced(masked_a, narrow_a, "yxz")
    narrow_grad_a = over_cores(matmul(masked_a, w_ea))
    grad_ra = reduced(layer, narrow_grad_a, "xyz")
    grad_in = (middle_wide + contract_cols(narrow_grad_a, w_ra)).astype(BF16)
    cross_b = contract_cols(narrow_b, w_eb)
    grad_base = (grad_wide * cross_b + middle_wide * cross_a).astype(BF16)
    return (spread_out(grad_in), spread_out(grad_base), grad_ra, grad_ea, grad_rb, grad_eb)


def solution(mesh):
    fsdp = mesh.shape["fsdp"]
    assert mesh.shape["rep"] == 4 and fsdp > 1 and fsdp & (fsdp - 1) == 0
    wide, narrow = P(("fsdp", "rep"), None), P("fsdp", None)
    return jax.shard_map(
        on_device,
        mesh=mesh,
        in_specs=(wide,) * 3 + (narrow,) * 4,
        out_specs=(wide,) * 2 + (narrow,) * 4,
        check_vma=False,
    )
```
